32 devices in a mesh: pipe: 4 (over x, core), mp: 8 (over z, y).
Axes of the slice: x: 2, y: 2, z: 4, core: 2. Of those that a mesh axis runs over, the one named last changes fastest.
Arguments:
- hidden_in: bfloat16 [32, 8192], P(None, 'mp'), may hold values from -24000 to 24000
- lengths: int32 [32], replicated, may hold values from 1 to 256
- assign: int32 [32], replicated, may hold values from 0 to 31, each once
- token_ids: int32 [32], replicated, may hold values from 0 to 12287
- attn_gain: bfloat16 [4, 8192], P('pipe', 'mp'), may hold values from 0.099609375 to 1.8984375
- qkv_weight: bfloat16 [4, 8192, 5120], P('pipe', 'mp'), may hold values from -0.0625 to 0.0625
- qkv_bias: bfloat16 [4, 5120], P('pipe'), may hold values from -3 to 3
- out_weight: bfloat16 [4, 4096, 8192], P('pipe', None, 'mp'), may hold values from -0.375 to 0.375
- kv_cache: bfloat16 [4, 32, 2, 4, 256, 128], P('pipe', 'mp'), may hold values from -120 to 120
- final_gain: bfloat16 [8192], P('mp'), may hold values from 0.099609375 to 1.8984375
- head_weight: bfloat16 [8192, 12288], P(None, ('pipe', 'mp')), may hold values from -0.9923308 to 0.9923308
Outputs:
- logprobs: float32 [32, 12288], P(None, ('pipe', 'mp'))
- chosen: float32 [32], replicated
The draws below stay inside these ranges and needn't reach their ends.
Inputs may be any that keep to these rules, and one draw needn't show every extreme that they name: `assign`: a permutation of the 32 requests.
All inputs are finite; a program needn't handle non-finite values.
Results may differ from the reference program's by a relative error of at most 0.0017.
Values may be sent and summed in bfloat16 or wider, within the bound.
A program may use at most 64 MiB of HBM per device.

```python
import math
import jax
import jax.numpy as jnp
import numpy as np
from jax import lax

D = 8192
HEADS = 32
KV_HEADS = 4
HEAD_DIM = 128
LEN = 256
LAYERS = 4
REQ = 32
QKV = 5120
VOCAB = 12288


def draw_kv_cache(key, part):
    base_draw = jnp.clip(jax.random.normal(jax.random.fold_in(key, 11), (LAYERS, REQ, 2, KV_HEADS, LEN, HEAD_DIM), jnp.float32), -4.0, 4.0)
    return base_draw.astype(jnp.bfloat16)


def column_profile(low_end, high_end):
    fraction = jnp.arange(D).astype(jnp.float32) / max(D - 1, 1)
    return low_end * jnp.exp(fraction * jnp.log(high_end / low_end))


def profiled_base(key):
    base_draw = jnp.clip(jax.random.normal(jax.random.fold_in(key, 21), (REQ, D), jnp.float32), -6.0, 6.0)
    profile = column_profile(3.0, 30.0)
    return base_draw * profile[None, :]


def draw_hidden_in(key, part):
    base_draw = profiled_base(key)
    return base_draw.astype(jnp.bfloat16)


def draw_head_weight(key, part):
    base_draw = jnp.clip(jax.random.normal(jax.random.fold_in(key, 24), (D, VOCAB), jnp.float32), -6.0, 6.0) * (3.0 * D ** (-0.5))
    return base_draw.astype(jnp.bfloat16)


def place_ends(drawn, rng, low, largest):
    place = [jax.random.randint(jax.random.fold_in(rng, axis), (), 0, length) for axis, length in enumerate(drawn.shape)]
    longest = drawn.shape.index(max(drawn.shape))
    neighbour = place[:longest] + [(place[longest] + 1) % drawn.shape[longest]] + place[longest + 1:]
    return drawn.at[tuple(place)].set(low).at[tuple(neighbour)].set(largest)


def block_scale(key, shape, pieces, least, high):
    def one(axis_at, parts):
        heights = jax.random.uniform(jax.random.fold_in(jax.random.fold_in(key, 6), axis_at), (parts,), jnp.float32, least / len(pieces), high / len(pieces))
        return jnp.repeat(jnp.exp(heights), shape[axis_at] // parts).reshape((-1,) + (1,) * (len(shape) - axis_at - 1))

    level = one(*pieces[0])
    for cut in pieces[1:]:
        level = level * one(*cut)
    return level


def rank_table(count, lean):
    portions = [(1 << 20) // math.isqrt(standing ** lean) + 1 for standing in range(1, count + 1)]
    scale = 1 + sum(portions) // (1 << 30)
    return np.cumsum(np.array([max(1, weight // scale) for weight in portions]))


def ranked_ids(own_key, extent, count, lean):
    table = rank_table(count, lean)
    ticket = jax.random.randint(jax.random.fold_in(own_key, 1), extent, 0, int(table[count - 1]))
    rank = jnp.searchsorted(jnp.asarray(table, jnp.int32), ticket, side="right")
    return jax.random.permutation(jax.random.fold_in(own_key, 2), count)[rank].astype(jnp.int32)


def bell_draw(own_key, shape, spread, bound, pieces=(), held_as=jnp.bfloat16):
    drawn = jax.random.normal(own_key, shape, jnp.float32) * spread
    if len(pieces) > 0:
        drawn = block_scale(own_key, shape, pieces, -0.22, 0.18) * drawn
    return jnp.clip(drawn, min=-bound, max=bound).astype(held_as)


def setup_inputs(seed: int = 0) -> dict:
    keys = jax.random.split(jax.random.key(seed), 12)
    return {
        "hidden_in": draw_hidden_in(jax.random.fold_in(keys[11], 71), 0),
        "lengths": place_ends(jax.random.randint(keys[1], (REQ,), 1, LEN + 1), jax.random.fold_in(keys[1], 1), 1, LEN).astype(jnp.int32),
        "assign": jax.random.permutation(keys[2], REQ).astype(jnp.int32),
        "token_ids": place_ends(ranked_ids(keys[3], (REQ,), VOCAB, 2), jax.random.fold_in(keys[3], 3), 0, VOCAB - 1).astype(jnp.int32),
        "attn_gain": jnp.clip(1.0 + 0.18 * jax.random.normal(keys[4], (LAYERS, D), jnp.float32), 0.099609375, 1.8984375).astype(jnp.bfloat16),
        "qkv_weight": bell_draw(keys[5], (LAYERS, D, QKV), D ** -0.5, 0.0625, ((0, 4), (1, 8))),
        "qkv_bias": bell_draw(keys[6], (LAYERS, QKV), 0.5, 3.0, ((0, 4),)),
        "out_weight": bell_draw(keys[7], (LAYERS, HEADS * HEAD_DIM, D), (HEADS * HEAD_DIM // 16) ** -0.5, 0.375, ((0, 4), (2, 8))),
        "kv_cache": draw_kv_cache(jax.random.fold_in(keys[11], 71), 0),
        "final_gain": jnp.clip(1.0 + 0.18 * jax.random.normal(keys[9], (D,), jnp.float32), 0.099609375, 1.8984375).astype(jnp.bfloat16),
        "head_weight": draw_head_weight(jax.random.fold_in(keys[11], 71), 0),
    }


EPS = 1e-06
THETA = 1000000.0

def rounded(values_in):
    return lax.optimization_barrier(values_in.astype(jnp.bfloat16)).astype(jnp.float32)

def rotate(values_in, positions):
    half_dim = values_in.shape[-1] // 2
    frequency = THETA ** (-jnp.arange(half_dim).astype(jnp.float32) * 2.0 / values_in.shape[-1])
    angles = positions.astype(jnp.float32)[:, None, None] * frequency[None, None, :]
    front_half = values_in[..., :half_dim]
    back_half = values_in[..., half_dim:]
    cosine = jnp.cos(angles)
    sine_part = jnp.sin(angles)
    return jnp.concatenate([front_half * cosine - back_half * sine_part, back_half * cosine + front_half * sine_part], axis=-1)

def reference(hidden_in, lengths, assign, token_ids, attn_gain, qkv_weight, qkv_bias, out_weight, kv_cache, final_gain, head_weight):
    stream = hidden_in[assign]
    positions = lengths[assign]
    group_size = HEADS // KV_HEADS
    query_cols = HEADS * HEAD_DIM
    key_cols = KV_HEADS * HEAD_DIM
    row_count = stream.shape[0]
    scale_factor = HEAD_DIM ** (-0.5)
    visible = jnp.arange(LEN).astype(jnp.int32)[None, :] < positions[:, None]
    key_mask = visible[:, None, None, :]
    for layer_index in range(LAYERS):
        current = stream.astype(jnp.float32)
        mean_sq = lax.optimization_barrier(jnp.mean(current * current, axis=1))
        scaled = (current * attn_gain[layer_index].astype(jnp.float32)).astype(jnp.bfloat16)
        projected = jnp.dot(scaled, qkv_weight[layer_index], preferred_element_type=jnp.float32)
        projected = projected * lax.rsqrt(mean_sq + EPS)[:, None] + qkv_bias[layer_index].astype(jnp.float32)
        queries = rotate(projected[:, :query_cols].reshape(row_count, HEADS, HEAD_DIM), positions).astype(jnp.bfloat16)
        key_new = rotate(projected[:, query_cols:query_cols + key_cols].reshape(row_count, KV_HEADS, HEAD_DIM), positions).astype(jnp.bfloat16)
        value_new = projected[:, query_cols + key_cols:].reshape(row_count, KV_HEADS, HEAD_DIM).astype(jnp.bfloat16)
        cache_rows = kv_cache[layer_index][assign].astype(jnp.float32)
        query_f = queries.astype(jnp.float32).reshape(row_count, KV_HEADS, group_size, HEAD_DIM)
        scores = jnp.einsum('rkgd,rkjd->rkgj', query_f, cache_rows[:, 0]) * scale_factor
        self_score = jnp.einsum('rkgd,rkd->rkg', query_f, key_new.astype(jnp.float32)) * scale_factor
        row_top = jnp.maximum(lax.optimization_barrier(jnp.max(jnp.where(key_mask, scores, -1e+30), axis=-1)), self_score)
        weights = jnp.where(key_mask, jnp.exp(scores - row_top[..., None]), 0.0)
        self_weight = jnp.exp(self_score - row_top)
        row_total = lax.optimization_barrier(jnp.sum(weights, axis=-1)) + self_weight
        summed = jnp.einsum('rkgj,rkjd->rkgd', rounded(weights), cache_rows[:, 1])
        summed = summed + rounded(self_weight)[..., None] * value_new.astype(jnp.float32)[:, :, None, :]
        attended = (summed / row_total[..., None]).astype(jnp.bfloat16).reshape(row_count, query_cols)
        update = jnp.dot(attended, out_weight[layer_index], preferred_element_type=jnp.float32)
        stream = (current + update).astype(jnp.bfloat16)
    current = stream.astype(jnp.float32)
    mean_sq = lax.optimization_barrier(jnp.mean(current * current, axis=1))
    normed = (current * final_gain.astype(jnp.float32) * lax.rsqrt(mean_sq + EPS)[:, None]).astype(jnp.bfloat16)
    logits = jnp.dot(normed, head_weight, preferred_element_type=jnp.float32)
    row_top = lax.optimization_barrier(jnp.max(logits, axis=1))
    row_total = lax.optimization_barrier(jnp.sum(jnp.exp(logits - row_top[:, None]), axis=1))
    logprobs = logits - (row_top + jnp.log(row_total))[:, None]
    targets = token_ids[assign]
    chosen = jnp.take_along_axis(logprobs, targets[:, None], axis=1)[:, 0]
    return (logprobs, chosen)
```

```python
import functools

import jax
import jax.numpy as jnp
import numpy as np
from jax import lax
from jax.experimental import pallas as pl
from jax.experimental.pallas import tpu as pltpu
from jax.sharding import PartitionSpec as P

HEADS = 32
KV_HEADS = 4
HEAD_DIM = 128
EPS = 1e-06
THETA = 1000000.0
MESH = pl.DeviceIdType.MESH
F32 = jnp.float32
BF16 = jnp.bfloat16


def remote(src, dst, send_sem, recv_sem, device):
    return pltpu.make_async_remote_copy(
        src_ref=src,
        dst_ref=dst,
        send_sem=send_sem,
        recv_sem=recv_sem,
        device_id=device,
        device_id_type=MESH,
    )


def kernel(
    sections,
    n,
    hidden,
    lengths,
    assign,
    token_ids,
    gain,
    qkv_weight,
    bias,
    out_weight,
    cache,
    final_gain,
    head_weight,
    freq,
    out,
    chosen,
    wq,
    wo,
    kv,
    hw,
    x,
    xo,
    scaled,
    part,
    part_in,
    sq,
    sq_in,
    bias_rows,
    att,
    att_in,
    att_rows,
    att_mat,
    fin,
    fsq,
    fsq_in,
    red,
    red_in,
    wq_sem,
    w_sem,
    part_s,
    part_r,
    sq_s,
    sq_r,
    att_s,
    att_r,
    hop_s,
    hop_r,
    fin_s,
    fin_r,
    fsq_s,
    fsq_r,
    fp_s,
    fp_r,
    red_s,
    red_r,
):
    sec = lax.axis_index("pipe")
    me = lax.axis_index("mp")
    total = sections * n
    rows, width = hidden.shape
    lc = kv.shape[0]
    heads_all = HEADS + 2 * KV_HEADS
    group = HEADS // KV_HEADS
    last = sections - 1
    scale = HEAD_DIM ** (-0.5)
    chunks = wq_sem.shape[0]
    cw = wq.shape[1] // chunks

    def wq_copy(c):
        cols = pl.ds(pl.multiple_of(c * cw, cw), cw)
        return pltpu.make_async_copy(qkv_weight.at[0, :, cols], wq.at[:, cols], wq_sem.at[c])

    for c in range(chunks):
        wq_copy(c).start()
    kv_copy = pltpu.make_async_copy(cache.at[0], kv, w_sem.at[0])
    wo_copy = pltpu.make_async_copy(out_weight.at[0], wo, w_sem.at[1])
    hw_copy = pltpu.make_async_copy(head_weight, hw, w_sem.at[2])
    kv_copy.start()
    wo_copy.start()
    hw_copy.start()

    barrier = pltpu.get_barrier_semaphore()
    mine = sec * n + me

    def greet(k, carry):
        other = lax.rem(mine + k, total)
        pl.semaphore_signal(
            barrier, inc=1, device_id=(other // n, lax.rem(other, n)), device_id_type=MESH
        )
        return carry

    lax.fori_loop(1, total, greet, 0)

    for i in range(heads_all):
        bias_rows[i : i + 1, :] = bias[:, i * HEAD_DIM : (i + 1) * HEAD_DIM].astype(F32)
    eye = lax.broadcasted_iota(jnp.int32, (rows, 128), 0) == lax.broadcasted_iota(
        jnp.int32, (rows, 128), 1
    )

    def to_row(col):
        return jnp.sum(jnp.where(eye, col, 0.0), axis=0, keepdims=True)

    def to_col(row):
        return jnp.sum(jnp.where(eye, row, 0.0), axis=1, keepdims=True)

    small_eye = lax.broadcasted_iota(jnp.int32, (rows, rows), 0) == lax.broadcasted_iota(
        jnp.int32, (rows, rows), 1
    )
    assign_col = jnp.sum(
        jnp.where(small_eye, assign[...].astype(F32), 0.0), axis=1, keepdims=True
    )
    order = assign_col == lax.broadcasted_iota(jnp.int32, (rows, rows), 1).astype(F32)
    target = jnp.sum(
        jnp.where(order, token_ids[...].astype(F32), 0.0), axis=1, keepdims=True
    )
    lane = lax.broadcasted_iota(jnp.int32, (1, HEAD_DIM), 1)
    lane_rows = lax.broadcasted_iota(jnp.int32, (1, rows), 1)
    own_len = [
        jnp.sum(
            jnp.where(lane_rows == me * lc + i, lengths[...].astype(F32), 0.0),
            axis=1,
            keepdims=True,
        )
        for i in range(lc)
    ]
    angles = jnp.concatenate([length * freq[...] for length in own_len], axis=0)
    cosine = jnp.cos(angles)
    sine = jnp.sin(angles) * jnp.where(lane < HEAD_DIM // 2, -1.0, 1.0)

    pl.semaphore_wait(barrier, total - 1)

    @pl.when(sec == 0)
    def _():
        x[...] = hidden[...]

    @pl.when(sec > 0)
    def _():
        remote(xo, x, hop_s, hop_r, (sec - 1, me)).wait_recv()

    current = x[...].astype(F32)
    sq[...] = jnp.broadcast_to(
        to_row(jnp.sum(current * current, axis=1, keepdims=True)), sq.shape
    )
    scaled[...] = (current * gain[...].astype(F32)).astype(BF16)

    def sq_copy(peer, slot, sem):
        return remote(sq, sq_in.at[slot], sq_s.at[peer], sq_r.at[sem], (sec, peer))

    for k in range(1, n):
        peer = lax.rem(me + k, n)
        sq_copy(peer, me, me).start()

    per = cw // HEAD_DIM

    def project(c, carry):
        wq_copy(c).wait()
        cols = pl.ds(pl.multiple_of(c * cw, cw), cw)
        piece = jnp.dot(scaled[...], wq[:, cols], preferred_element_type=F32)
        for j in range(per):
            part[pl.ds(c * per + j, rows, stride=heads_all), :] = piece[
                :, j * HEAD_DIM : (j + 1) * HEAD_DIM
            ]
        return carry

    lax.fori_loop(0, chunks, project, 0)

    block = lc * heads_all

    def part_copy(peer, slot):
        return remote(
            part.at[pl.ds(pl.multiple_of(peer * block, block), block), :],
            part_in.at[slot],
            part_s.at[peer],
            part_r.at[slot],
            (sec, peer),
        )

    for k in range(1, n):
        part_copy(lax.rem(me + k, n), me).start()

    squares = sq[...]
    for k in range(1, n):
        peer = lax.rem(me + n - k, n)
        sq_copy(peer, peer, peer).wait_recv()
        squares = squares + sq_in[peer]
    summed_cols = part[pl.ds(pl.multiple_of(me * block, block), block), :]
    for k in range(1, n):
        peer = lax.rem(me + n - k, n)
        part_copy(peer, peer).wait_recv()
        summed_cols = summed_cols + part_in[peer]
    kv_copy.wait()
    pos = lax.broadcasted_iota(jnp.int32, (1, kv.shape[3]), 1).astype(F32)
    for i in range(lc):
        mean = (
            jnp.sum(
                jnp.where(lane == me * lc + i, squares[0:1, :], 0.0), axis=1, keepdims=True
            )
            / (n * width)
        )
        rows_i = summed_cols[i * heads_all : (i + 1) * heads_all] * lax.rsqrt(
            mean + EPS
        ) + bias_rows[...]
        turned = (
            rows_i * cosine[i : i + 1]
            + pltpu.roll(rows_i, HEAD_DIM // 2, 1) * sine[i : i + 1]
        )
        visible = pos < own_len[i]
        heads = []
        for h in range(KV_HEADS):
            query = turned[h * group : (h + 1) * group].astype(BF16)
            key_new = turned[HEADS + h : HEADS + h + 1].astype(BF16).astype(F32)
            at = HEADS + KV_HEADS + h
            value_new = rows_i[at : at + 1].astype(BF16).astype(F32)
            scores = (
                lax.dot_general(
                    query,
                    kv[i, 0, h],
                    (((1,), (1,)), ((), ())),
                    preferred_element_type=F32,
                )
                * scale
            )
            self_score = (
                jnp.sum(query.astype(F32) * key_new, axis=1, keepdims=True) * scale
            )
            top = jnp.maximum(
                jnp.max(jnp.where(visible, scores, -1e30), axis=1, keepdims=True), self_score
            )
            weights = jnp.where(visible, jnp.exp(scores - top), 0.0)
            self_weight = jnp.exp(self_score - top)
            denominator = jnp.sum(weights, axis=1, keepdims=True) + self_weight
            mixed = jnp.dot(weights.astype(BF16), kv[i, 1, h], preferred_element_type=F32)
            mixed = mixed + self_weight.astype(BF16).astype(F32) * value_new
            heads.append(mixed / denominator)
        att[i * HEADS : (i + 1) * HEADS, :] = jnp.concatenate(heads, axis=0).astype(BF16)

    def att_copy(peer, slot):
        return remote(att, att_in.at[slot], att_s.at[peer], att_r.at[slot], (sec, peer))

    for k in range(1, n):
        att_copy(lax.rem(me + k, n), me).start()
    span = lc * HEADS
    att_rows[pl.ds(pl.multiple_of(me * span, span), span), :] = att[...].astype(F32)
    for k in range(1, n):
        peer = lax.rem(me + n - k, n)
        att_copy(peer, peer).wait_recv()
        att_rows[pl.ds(pl.multiple_of(peer * span, span), span), :] = att_in[peer].astype(F32)
    for i in range(HEADS):
        att_mat[:, i * HEAD_DIM : (i + 1) * HEAD_DIM] = att_rows[
            pl.ds(i, rows, stride=HEADS), :
        ].astype(BF16)
    wo_copy.wait()
    ow = min(256, width)

    def project_out(c, carry):
        cols = pl.ds(pl.multiple_of(c * ow, ow), ow)
        update = jnp.dot(att_mat[...], wo[:, cols], preferred_element_type=F32)
        xo[:, cols] = (x[:, cols].astype(F32) + update).astype(BF16)
        return carry

    lax.fori_loop(0, width // ow, project_out, 0)

    @pl.when(sec < last)
    def _():
        hop = remote(xo, x, hop_s, hop_r, (sec + 1, me))
        hop.start()
        hop.wait_send()

    def fin_pipe(k, from_here):
        to = lax.rem(sec + k, sections)
        dev = (to, me)
        return (
            remote(fin.at[me], fin.at[me], fp_s.at[2 * k], fp_r.at[0], dev),
            remote(fsq_in.at[me], fsq_in.at[me], fp_s.at[2 * k + 1], fp_r.at[1], dev),
        )

    @pl.when(sec == last)
    def _():
        final = jnp.dot(order.astype(BF16), xo[...], preferred_element_type=F32)
        fin[me] = (final * final_gain[...].astype(F32)).astype(BF16)
        fsq_in[me] = jnp.broadcast_to(
            to_row(jnp.sum(final * final, axis=1, keepdims=True)), fsq.shape
        )
        for k in range(1, sections):
            for copy in fin_pipe(k, True):
                copy.start()

    @pl.when(sec < last)
    def _():
        for copy in fin_pipe(1, False):
            copy.wait_recv()

    def fin_copy(peer, slot):
        return remote(
            fin.at[slot], fin.at[slot], fin_s.at[peer], fin_r.at[slot], (sec, peer)
        )

    def fsq_copy(peer, slot):
        return remote(
            fsq_in.at[slot], fsq_in.at[slot], fsq_s.at[peer], fsq_r.at[slot], (sec, peer)
        )

    for k in range(1, n):
        peer = lax.rem(me + k, n)
        fin_copy(peer, me).start()
        fsq_copy(peer, me).start()
    hw_copy.wait()

    def head(k, logits):
        peer = lax.rem(me + n - k, n)

        @pl.when(k > 0)
        def _():
            fin_copy(peer, peer).wait_recv()

        rows_at = pl.ds(pl.multiple_of(peer * width, width), width)
        return logits + jnp.dot(fin[peer], hw[rows_at, :], preferred_element_type=F32)

    logits = lax.fori_loop(0, n, head, jnp.zeros(out.shape, F32))
    squares = fsq_in[me]
    for k in range(1, n):
        peer = lax.rem(me + n - k, n)
        fsq_copy(peer, peer).wait_recv()
        squares = squares + fsq_in[peer]
    logits = logits * lax.rsqrt(to_col(squares[0:1, :]) / (n * width) + EPS)
    vocab = out.shape[1]
    ids = (mine * vocab + lax.broadcasted_iota(jnp.int32, (1, vocab), 1)).astype(F32)
    picked = jnp.sum(jnp.where(ids == target, logits, 0.0), axis=1, keepdims=True)
    top = jnp.max(logits, axis=1, keepdims=True)
    amount = jnp.sum(jnp.exp(logits - top), axis=1, keepdims=True)
    red[...] = jnp.concatenate(
        [to_row(top), to_row(amount), to_row(picked), jnp.zeros((5, 128), F32)], axis=0
    )

    def red_copy(other, slot):
        return remote(
            red,
            red_in.at[slot],
            red_s.at[other],
            red_r.at[slot],
            (other // n, lax.rem(other, n)),
        )

    def red_start(k, carry):
        red_copy(lax.rem(mine + k, total), mine).start()
        return carry

    lax.fori_loop(1, total, red_start, 0)
    red_in[mine] = red[...]

    def red_wait(k, carry):
        other = lax.rem(mine + total - k, total)
        red_copy(other, other).wait_recv()
        return carry

    lax.fori_loop(1, total, red_wait, 0)
    tops = red_in[:, 0, :]
    row_top = jnp.max(tops, axis=0, keepdims=True)
    row_total = jnp.sum(red_in[:, 1, :] * jnp.exp(tops - row_top), axis=0, keepdims=True)
    log_total = row_top + jnp.log(row_total)
    chosen[...] = jnp.sum(red_in[:, 2, :], axis=0, keepdims=True) - log_total
    out[...] = logits - to_col(log_total)

    for k in range(1, n):
        peer = lax.rem(me + k, n)
        sq_copy(peer, me, me).wait_send()
        part_copy(peer, me).wait_send()
        att_copy(peer, me).wait_send()
        fin_copy(peer, me).wait_send()
        fsq_copy(peer, me).wait_send()

    @pl.when(sec == last)
    def _():
        for k in range(1, sections):
            for copy in fin_pipe(k, True):
                copy.wait_send()

    def red_done(k, carry):
        red_copy(lax.rem(mine + k, total), mine).wait_send()
        return carry

    lax.fori_loop(1, total, red_done, 0)


def local(
    hidden_in,
    lengths,
    assign,
    token_ids,
    attn_gain,
    qkv_weight,
    qkv_bias,
    out_weight,
    kv_cache,
    final_gain,
    head_weight,
):
    sections = lax.axis_size("pipe")
    n = lax.axis_size("mp")
    rows, width = hidden_in.shape
    lc = kv_cache.shape[1]
    qkv = qkv_weight.shape[2]
    inner = out_weight.shape[1]
    vocab = head_weight.shape[1]
    heads_all = HEADS + 2 * KV_HEADS
    half = HEAD_DIM // 2
    frequency = np.float32(THETA) ** (
        -np.arange(half).astype(np.float32) * np.float32(2.0) / np.float32(HEAD_DIM)
    )
    freq = jnp.asarray(np.concatenate([frequency, frequency])[None, :], F32)
    chunks = qkv // 512
    dma = pltpu.SemaphoreType.DMA
    vm = pl.BlockSpec(memory_space=pltpu.VMEM)
    hbm = pl.BlockSpec(memory_space=pl.ANY)
    total = sections * n
    logprobs, chosen = pl.pallas_call(
        functools.partial(kernel, sections, n),
        out_shape=(
            jax.ShapeDtypeStruct((rows, vocab), F32),
            jax.ShapeDtypeStruct((1, 128), F32),
        ),
        in_specs=[vm, vm, vm, vm, vm, hbm, vm, hbm, hbm, vm, hbm, vm],
        out_specs=(vm, vm),
        scratch_shapes=[
            pltpu.VMEM((width, qkv), BF16),
            pltpu.VMEM((inner, width), BF16),
            pltpu.VMEM(kv_cache.shape[1:], BF16),
            pltpu.VMEM(head_weight.shape, BF16),
            pltpu.VMEM((rows, width), BF16),
            pltpu.VMEM((rows, width), BF16),
            pltpu.VMEM((rows, width), BF16),
            pltpu.VMEM((rows * heads_all, HEAD_DIM), F32),
            pltpu.VMEM((n, lc * heads_all, HEAD_DIM), F32),
            pltpu.VMEM((8, 128), F32),
            pltpu.VMEM((n, 8, 128), F32),
            pltpu.VMEM((heads_all, HEAD_DIM), F32),
            pltpu.VMEM((lc * HEADS, HEAD_DIM), BF16),
            pltpu.VMEM((n, lc * HEADS, HEAD_DIM), BF16),
            pltpu.VMEM((rows * HEADS, HEAD_DIM), F32),
            pltpu.VMEM((rows, inner), BF16),
            pltpu.VMEM((n, rows, width), BF16),
            pltpu.VMEM((8, 128), F32),
            pltpu.VMEM((n, 8, 128), F32),
            pltpu.VMEM((8, 128), F32),
            pltpu.VMEM((total, 8, 128), F32),
            dma((chunks,)),
            dma((3,)),
            dma((n,)),
            dma((n,)),
            dma((n,)),
            dma((n,)),
            dma((n,)),
            dma((n,)),
            dma,
            dma,
            dma((n,)),
            dma((n,)),
            dma((n,)),
            dma((n,)),
            dma((2 * sections,)),
            dma((2,)),
            dma((total,)),
            dma((total,)),
        ],
        compiler_params=pltpu.CompilerParams(
            collective_id=0, has_side_effects=True, vmem_limit_bytes=60 * 1024 * 1024
        ),
    )(
        hidden_in,
        lengths.reshape(1, rows),
        assign.reshape(1, rows),
        token_ids.reshape(1, rows),
        attn_gain,
        qkv_weight,
        qkv_bias,
        out_weight,
        kv_cache,
        final_gain.reshape(1, width),
        head_weight,
        freq,
    )
    return logprobs, chosen[0, :rows]


def solution(mesh):
    return jax.shard_map(
        local,
        mesh=mesh,
        in_specs=(
            P(None, "mp"),
            P(),
            P(),
            P(),
            P("pipe", "mp"),
            P("pipe", "mp", None),
            P("pipe", None),
            P("pipe", None, "mp"),
            P("pipe", "mp", None, None, None, None),
            P("mp"),
            P(None, ("pipe", "mp")),
        ),
        out_specs=(P(None, ("pipe", "mp")), P()),
        check_vma=False,
    )
```

```python
import functools

import jax
import jax.numpy as jnp
import numpy as np
from jax import lax
from jax.experimental import pallas as pl
from jax.experimental.pallas import tpu as pltpu
from jax.sharding import PartitionSpec as P

HEADS = 32
KV_HEADS = 4
HEAD_DIM = 128
EPS = 1e-06
THETA = 1000000.0
MESH = pl.DeviceIdType.MESH
F32 = jnp.float32
BF16 = jnp.bfloat16


def remote(src, dst, send_sem, recv_sem, device):
    return pltpu.make_async_remote_copy(
        src_ref=src,
        dst_ref=dst,
        send_sem=send_sem,
        recv_sem=recv_sem,
        device_id=device,
        device_id_type=MESH,
    )


def kernel(
    sections,
    n,
    hidden,
    lengths,
    assign,
    token_ids,
    gain,
    qkv_weight,
    bias,
    out_weight,
    cache,
    final_gain,
    head_weight,
    freq,
    out,
    chosen,
    wq,
    wo,
    kv,
    hw,
    x,
    xo,
    scaled,
    stage,
    part,
    part_in,
    sq,
    sq_in,
    bias_rows,
    fresh,
    att,
    att_in,
    update,
    fin,
    fsq_in,
    red,
    red_in,
    wq_sem,
    w_sem,
    part_s,
    part_r,
    sq_s,
    sq_r,
    att_s,
    att_r,
    hop_s,
    hop_r,
    fin_s,
    fin_r,
    sib_s,
    sib_r,
    fsq_s,
    fsq_r,
    fp_s,
    fp_r,
    red_s,
    red_r,
):
    sec = lax.axis_index("pipe")
    me = lax.axis_index("mp")
    total = sections * n
    rows, width = hidden.shape
    lc = kv.shape[0]
    heads_all = HEADS + 2 * KV_HEADS
    group = HEADS // KV_HEADS
    phases = heads_all // group
    span = lc * group
    last = sections - 1
    scale = HEAD_DIM ** (-0.5)
    cw = group * HEAD_DIM
    half = rows // 2
    core = lax.rem(sec, 2)
    sibling = sec + 1 - 2 * core

    def wq_copy(c):
        cols = pl.ds(pl.multiple_of(c * cw, cw), cw)
        return pltpu.make_async_copy(qkv_weight.at[0, :, cols], wq.at[:, cols], wq_sem.at[c])

    def phase_of(k):
        return lax.rem(k + phases - 1, phases)

    for k in range(phases):
        wq_copy((k + phases - 1) % phases).start()
    kv_copy = pltpu.make_async_copy(cache.at[0], kv, w_sem.at[0])
    wo_copy = pltpu.make_async_copy(out_weight.at[0], wo, w_sem.at[1])
    hw_copy = pltpu.make_async_copy(head_weight, hw, w_sem.at[2])

    @pl.when(sec > 0)
    def _():
        kv_copy.start()
        wo_copy.start()
        hw_copy.start()

    barrier = pltpu.get_barrier_semaphore()
    mine = sec * n + me

    def greet(k, carry):
        other = lax.rem(mine + k, total)
        pl.semaphore_signal(
            barrier, inc=1, device_id=(other // n, lax.rem(other, n)), device_id_type=MESH
        )
        return carry

    lax.fori_loop(1, total, greet, 0)

    for i in range(heads_all):
        bias_rows[i : i + 1, :] = bias[:, i * HEAD_DIM : (i + 1) * HEAD_DIM].astype(F32)
    eye = lax.broadcasted_iota(jnp.int32, (rows, 128), 0) == lax.broadcasted_iota(
        jnp.int32, (rows, 128), 1
    )

    def to_row(col):
        return jnp.sum(jnp.where(eye, col, 0.0), axis=0, keepdims=True)

    def to_col(row):
        return jnp.sum(jnp.where(eye, row, 0.0), axis=1, keepdims=True)

    small_eye = lax.broadcasted_iota(jnp.int32, (rows, rows), 0) == lax.broadcasted_iota(
        jnp.int32, (rows, rows), 1
    )
    assign_col = jnp.sum(
        jnp.where(small_eye, assign[...].astype(F32), 0.0), axis=1, keepdims=True
    )
    order = assign_col == lax.broadcasted_iota(jnp.int32, (rows, rows), 1).astype(F32)
    target = jnp.sum(
        jnp.where(order, token_ids[...].astype(F32), 0.0), axis=1, keepdims=True
    )
    lane = lax.broadcasted_iota(jnp.int32, (1, HEAD_DIM), 1)
    lane_rows = lax.broadcasted_iota(jnp.int32, (1, rows), 1)
    own_len = [
        jnp.sum(
            jnp.where(lane_rows == me * lc + i, lengths[...].astype(F32), 0.0),
            axis=1,
            keepdims=True,
        )
        for i in range(lc)
    ]
    angles = jnp.concatenate([length * freq[...] for length in own_len], axis=0)
    cosine = jnp.cos(angles)
    sine = jnp.sin(angles) * jnp.where(lane < HEAD_DIM // 2, -1.0, 1.0)

    pl.semaphore_wait(barrier, total - 1)

    @pl.when(sec == 0)
    def _():
        x[...] = hidden[...]

    @pl.when(sec > 0)
    def _():
        remote(xo, x, hop_s, hop_r, (sec - 1, me)).wait_recv()

    current = x[...].astype(F32)
    sq[...] = jnp.broadcast_to(
        to_row(jnp.sum(current * current, axis=1, keepdims=True)), sq.shape
    )
    scaled[...] = (current * gain[...].astype(F32)).astype(BF16)

    def sq_copy(peer, slot):
        return remote(sq, sq_in.at[slot], sq_s.at[peer], sq_r.at[slot], (sec, peer))

    def to_peer(k):
        return lax.rem(me + k, n)

    for k in range(1, n):
        sq_copy(to_peer(k), me).start()
    sq_in[me] = sq[...]

    def part_copy(phase, peer, slot):
        return remote(
            part.at[phase, peer],
            part_in.at[phase, slot],
            part_s.at[phase, peer],
            part_r.at[phase, slot],
            (sec, peer),
        )

    def project(k, carry):
        phase = phase_of(k)
        wq_copy(phase).wait()
        base = pl.multiple_of(phase * cw, cw)
        piece = jnp.dot(scaled[...], wq[:, pl.ds(base, cw)], preferred_element_type=F32)
        for j in range(group):
            stage[pl.ds(j, rows, stride=group), :] = piece[
                :, j * HEAD_DIM : (j + 1) * HEAD_DIM
            ]
        for p in range(n):
            part[phase, p] = stage[p * span : (p + 1) * span, :].astype(BF16)
        for k in range(1, n):
            part_copy(phase, to_peer(k), me).start()
        part_in[phase, me] = part[phase, me]
        return carry

    lax.fori_loop(0, phases, project, 0)

    @pl.when(sec == 0)
    def _():
        kv_copy.start()
        wo_copy.start()
        hw_copy.start()

    def from_peer(k):
        return lax.rem(me + n - k, n)

    def summed(phase):
        for k in range(1, n):
            peer = from_peer(k)
            part_copy(phase, peer, peer).wait_recv()
        result = part_in[phase, 0].astype(F32)
        for p in range(1, n):
            result = result + part_in[phase, p].astype(F32)
        return result

    for k in range(1, n):
        peer = from_peer(k)
        sq_copy(peer, peer).wait_recv()
    squares = sq_in[0]
    for p in range(1, n):
        squares = squares + sq_in[p]
    factor = [
        lax.rsqrt(
            jnp.sum(
                jnp.where(lane == me * lc + i, squares[0:1, :], 0.0), axis=1, keepdims=True
            )
            / (n * width)
            + EPS
        )
        for i in range(lc)
    ]

    def turn(block, i):
        return (
            block * cosine[i : i + 1]
            + pltpu.roll(block, HEAD_DIM // 2, 1) * sine[i : i + 1]
        )

    is_key = lax.broadcasted_iota(jnp.int32, (2 * KV_HEADS, HEAD_DIM), 0) < KV_HEADS
    block_sum = summed(phases - 1)
    for i in range(lc):
        block = block_sum[i * group : (i + 1) * group] * factor[i] + bias_rows[HEADS:, :]
        fresh[i] = jnp.where(is_key, turn(block, i), block).astype(BF16).astype(F32)
    kv_copy.wait()
    pos = lax.broadcasted_iota(jnp.int32, (1, kv.shape[3]), 1).astype(F32)

    def att_copy(h, peer, slot):
        return remote(
            att.at[h], att_in.at[h, slot], att_s.at[h, peer], att_r.at[h, slot], (sec, peer)
        )

    def attend(h, carry):
        block_sum = summed(h)
        bias_h = bias_rows[pl.ds(pl.multiple_of(h * group, group), group), :]
        done = []
        for i in range(lc):
            block = block_sum[i * group : (i + 1) * group] * factor[i] + bias_h
            query = turn(block, i).astype(BF16)
            key_new = fresh[i, pl.ds(h, 1), :]
            value_new = fresh[i, pl.ds(KV_HEADS + h, 1), :]
            visible = pos < own_len[i]
            scores = (
                lax.dot_general(
                    query,
                    kv[i, 0, h],
                    (((1,), (1,)), ((), ())),
                    preferred_element_type=F32,
                )
                * scale
            )
            self_score = (
                jnp.sum(query.astype(F32) * key_new, axis=1, keepdims=True) * scale
            )
            top = jnp.maximum(
                jnp.max(jnp.where(visible, scores, -1e30), axis=1, keepdims=True), self_score
            )
            weights = jnp.where(visible, jnp.exp(scores - top), 0.0)
            self_weight = jnp.exp(self_score - top)
            denominator = jnp.sum(weights, axis=1, keepdims=True) + self_weight
            mixed = jnp.dot(weights.astype(BF16), kv[i, 1, h], preferred_element_type=F32)
            mixed = mixed + self_weight.astype(BF16).astype(F32) * value_new
            done.append(mixed / denominator)
        att[h] = jnp.concatenate(done, axis=0).astype(BF16)
        for k in range(1, n):
            att_copy(h, to_peer(k), me).start()
        att_in[h, me] = att[h]
        return carry

    lax.fori_loop(0, KV_HEADS, attend, 0)
    wo_copy.wait()
    update[...] = x[...].astype(F32)

    def project_out(h, carry):
        for k in range(1, n):
            peer = from_peer(k)
            att_copy(h, peer, peer).wait_recv()
        for p in range(n):
            stage[p * span : (p + 1) * span, :] = att_in[h, p].astype(F32)
        mat = jnp.concatenate(
            [stage[pl.ds(j, rows, stride=group), :].astype(BF16) for j in range(group)],
            axis=1,
        )
        depth = pl.ds(pl.multiple_of(h * cw, cw), cw)
        update[...] += jnp.dot(mat, wo[depth, :], preferred_element_type=F32)
        return carry

    lax.fori_loop(0, KV_HEADS, project_out, 0)
    xo[...] = update[...].astype(BF16)

    @pl.when(sec < last)
    def _():
        hop = remote(xo, x, hop_s, hop_r, (sec + 1, me))
        hop.start()
        hop.wait_send()

    def fin_pipe(k):
        to = lax.rem(sec + k, sections)
        piece = lax.rem(to, 2)
        return (
            remote(fin.at[piece, me], fin.at[piece, me], fp_s.at[2 * k], fp_r.at[0], (to, me)),
            remote(fsq_in.at[me], fsq_in.at[me], fp_s.at[2 * k + 1], fp_r.at[1], (to, me)),
        )

    @pl.when(sec == last)
    def _():
        final = jnp.dot(order.astype(BF16), xo[...], preferred_element_type=F32)
        both = (final * final_gain[...].astype(F32)).astype(BF16)
        fin[0, me] = both[:half]
        fin[1, me] = both[half:]
        fsq_in[me] = jnp.broadcast_to(
            to_row(jnp.sum(final * final, axis=1, keepdims=True)), (8, 128)
        )
        for k in range(1, sections):
            for copy in fin_pipe(k):
                copy.start()

    @pl.when(sec < last)
    def _():
        arriving = remote(fin.at[core, me], fin.at[core, me], fp_s.at[0], fp_r.at[0], (last, me))
        arriving.wait_recv()
        arriving = remote(fsq_in.at[me], fsq_in.at[me], fp_s.at[1], fp_r.at[1], (last, me))
        arriving.wait_recv()

    def fin_copy(peer, slot):
        return remote(
            fin.at[core, slot], fin.at[core, slot], fin_s.at[peer], fin_r.at[slot], (sec, peer)
        )

    def sib_copy(piece, slot):
        return remote(
            fin.at[piece, slot], fin.at[piece, slot], sib_s.at[slot], sib_r.at[slot], (sibling, me)
        )

    def fsq_copy(peer, slot):
        return remote(
            fsq_in.at[slot], fsq_in.at[slot], fsq_s.at[peer], fsq_r.at[slot], (sec, peer)
        )

    for k in range(1, n):
        fin_copy(to_peer(k), me).start()
    for k in range(1, n):
        fsq_copy(to_peer(k), me).start()

    @pl.when(sec < last - 1)
    def _():
        sib_copy(core, me).start()

    @pl.when(sec == last - 1)
    def _():
        mate = remote(fin.at[1 - core, me], fin.at[1 - core, me], fp_s.at[0], fp_r.at[2], (last, me))
        mate.wait_recv()

    @pl.when(sec == last)
    def _():
        mate = remote(
            fin.at[core, me], fin.at[core, me], sib_s.at[me], fp_r.at[2], (sibling, me)
        )
        mate.start()

    for k in range(1, n):
        peer = from_peer(k)
        fin_copy(peer, peer).wait_recv()
        sib_copy(core, peer).start()

    @pl.when(sec < last - 1)
    def _():
        sib_copy(1 - core, me).wait_recv()

    hw_copy.wait()

    def head(k, logits):
        peer = from_peer(k)

        @pl.when(k > 0)
        def _():
            sib_copy(1 - core, peer).wait_recv()

        rows_at = pl.ds(pl.multiple_of(peer * width, width), width)
        both = jnp.concatenate([fin[0, peer], fin[1, peer]], axis=0)
        return logits + jnp.dot(both, hw[rows_at, :], preferred_element_type=F32)

    logits = lax.fori_loop(0, n, head, jnp.zeros(out.shape, F32))
    for k in range(1, n):
        peer = from_peer(k)
        fsq_copy(peer, peer).wait_recv()
    squares = fsq_in[0]
    for p in range(1, n):
        squares = squares + fsq_in[p]
    logits = logits * lax.rsqrt(to_col(squares[0:1, :]) / (n * width) + EPS)
    vocab = out.shape[1]
    ids = (mine * vocab + lax.broadcasted_iota(jnp.int32, (1, vocab), 1)).astype(F32)
    picked = jnp.sum(jnp.where(ids == target, logits, 0.0), axis=1, keepdims=True)
    top = jnp.max(logits, axis=1, keepdims=True)
    amount = jnp.sum(jnp.exp(logits - top), axis=1, keepdims=True)
    red[...] = jnp.concatenate(
        [to_row(top), to_row(amount), to_row(picked), jnp.zeros((5, 128), F32)], axis=0
    )

    def red_copy(other, slot):
        return remote(
            red,
            red_in.at[slot],
            red_s.at[other],
            red_r.at[slot],
            (other // n, lax.rem(other, n)),
        )

    def red_start(k, carry):
        red_copy(lax.rem(mine + k, total), mine).start()
        return carry

    lax.fori_loop(1, total, red_start, 0)
    red_in[mine] = red[...]

    def red_wait(k, carry):
        other = lax.rem(mine + total - k, total)
        red_copy(other, other).wait_recv()
        return carry

    lax.fori_loop(1, total, red_wait, 0)
    tops = red_in[:, 0, :]
    row_top = jnp.max(tops, axis=0, keepdims=True)
    row_total = jnp.sum(red_in[:, 1, :] * jnp.exp(tops - row_top), axis=0, keepdims=True)
    log_total = row_top + jnp.log(row_total)
    chosen[...] = jnp.sum(red_in[:, 2, :], axis=0, keepdims=True) - log_total
    out[...] = logits - to_col(log_total)

    def peer_done(k, carry):
        peer = to_peer(k)
        sq_copy(peer, me).wait_send()
        for phase in range(phases):
            part_copy(phase, peer, me).wait_send()
        for h in range(KV_HEADS):
            att_copy(h, peer, me).wait_send()
        fin_copy(peer, me).wait_send()
        fsq_copy(peer, me).wait_send()
        sib_copy(core, peer).wait_send()
        return carry

    lax.fori_loop(1, n, peer_done, 0)

    @pl.when(sec != last - 1)
    def _():
        sib_copy(core, me).wait_send()

    @pl.when(sec == last)
    def _():
        for k in range(1, sections):
            for copy in fin_pipe(k):
                copy.wait_send()

    def red_done(k, carry):
        red_copy(lax.rem(mine + k, total), mine).wait_send()
        return carry

    lax.fori_loop(1, total, red_done, 0)


def local(
    hidden_in,
    lengths,
    assign,
    token_ids,
    attn_gain,
    qkv_weight,
    qkv_bias,
    out_weight,
    kv_cache,
    final_gain,
    head_weight,
):
    sections = lax.axis_size("pipe")
    n = lax.axis_size("mp")
    rows, width = hidden_in.shape
    lc = kv_cache.shape[1]
    qkv = qkv_weight.shape[2]
    inner = out_weight.shape[1]
    vocab = head_weight.shape[1]
    heads_all = HEADS + 2 * KV_HEADS
    half = HEAD_DIM // 2
    frequency = np.float32(THETA) ** (
        -np.arange(half).astype(np.float32) * np.float32(2.0) / np.float32(HEAD_DIM)
    )
    freq = jnp.asarray(np.concatenate([frequency, frequency])[None, :], F32)
    group = HEADS // KV_HEADS
    phases = heads_all // group
    span = lc * group
    dma = pltpu.SemaphoreType.DMA
    vm = pl.BlockSpec(memory_space=pltpu.VMEM)
    hbm = pl.BlockSpec(memory_space=pl.ANY)
    total = sections * n
    logprobs, chosen = pl.pallas_call(
        functools.partial(kernel, sections, n),
        out_shape=(
            jax.ShapeDtypeStruct((rows, vocab), F32),
            jax.ShapeDtypeStruct((1, 128), F32),
        ),
        in_specs=[vm, vm, vm, vm, vm, hbm, vm, hbm, hbm, vm, hbm, vm],
        out_specs=(vm, vm),
        scratch_shapes=[
            pltpu.VMEM((width, qkv), BF16),
            pltpu.VMEM((inner, width), BF16),
            pltpu.VMEM(kv_cache.shape[1:], BF16),
            pltpu.VMEM(head_weight.shape, BF16),
            pltpu.VMEM((rows, width), BF16),
            pltpu.VMEM((rows, width), BF16),
            pltpu.VMEM((rows, width), BF16),
            pltpu.VMEM((rows * group, HEAD_DIM), F32),
            pltpu.VMEM((phases, n, span, HEAD_DIM), BF16),
            pltpu.VMEM((phases, n, span, HEAD_DIM), BF16),
            pltpu.VMEM((8, 128), F32),
            pltpu.VMEM((n, 8, 128), F32),
            pltpu.VMEM((heads_all, HEAD_DIM), F32),
            pltpu.VMEM((lc, 2 * KV_HEADS, HEAD_DIM), F32),
            pltpu.VMEM((KV_HEADS, span, HEAD_DIM), BF16),
            pltpu.VMEM((KV_HEADS, n, span, HEAD_DIM), BF16),
            pltpu.VMEM((rows, width), F32),
            pltpu.VMEM((2, n, rows // 2, width), BF16),
            pltpu.VMEM((n, 8, 128), F32),
            pltpu.VMEM((8, 128), F32),
            pltpu.VMEM((total, 8, 128), F32),
            dma((phases,)),
            dma((3,)),
            dma((phases, n)),
            dma((phases, n)),
            dma((n,)),
            dma((n,)),
            dma((KV_HEADS, n)),
            dma((KV_HEADS, n)),
            dma,
            dma,
            dma((n,)),
            dma((n,)),
            dma((n,)),
            dma((n,)),
            dma((n,)),
            dma((n,)),
            dma((2 * sections,)),
            dma((3,)),
            dma((total,)),
            dma((total,)),
        ],
        compiler_params=pltpu.CompilerParams(
            collective_id=0, has_side_effects=True, vmem_limit_bytes=60 * 1024 * 1024
        ),
    )(
        hidden_in,
        lengths.reshape(1, rows),
        assign.reshape(1, rows),
        token_ids.reshape(1, rows),
        attn_gain,
        qkv_weight,
        qkv_bias,
        out_weight,
        kv_cache,
        final_gain.reshape(1, width),
        head_weight,
        freq,
    )
    return logprobs, chosen[0, :rows]


def solution(mesh):
    return jax.shard_map(
        local,
        mesh=mesh,
        in_specs=(
            P(None, "mp"),
            P(),
            P(),
            P(),
            P("pipe", "mp"),
            P("pipe", "mp", None),
            P("pipe", None),
            P("pipe", None, "mp"),
            P("pipe", "mp", None, None, None, None),
            P("mp"),
            P(None, ("pipe", "mp")),
        ),
        out_specs=(P(None, ("pipe", "mp")), P()),
        check_vma=False,
    )
```

```python
import functools

import jax
import jax.numpy as jnp
import numpy as np
from jax import lax
from jax.experimental import pallas as pl
from jax.experimental.pallas import tpu as pltpu
from jax.sharding import PartitionSpec as P

HEADS = 32
KV_HEADS = 4
HEAD_DIM = 128
EPS = 1e-06
THETA = 1000000.0
MESH = pl.DeviceIdType.MESH
F32 = jnp.float32
BF16 = jnp.bfloat16


def remote(src, dst, send_sem, recv_sem, device):
    return pltpu.make_async_remote_copy(
        src_ref=src,
        dst_ref=dst,
        send_sem=send_sem,
        recv_sem=recv_sem,
        device_id=device,
        device_id_type=MESH,
    )


def kernel(
    sections,
    n,
    hidden,
    lengths,
    assign,
    token_ids,
    gain,
    qkv_weight,
    bias,
    out_weight,
    cache,
    final_gain,
    head_weight,
    freq,
    out,
    chosen,
    wq,
    wo,
    kv,
    hw,
    x,
    xo,
    scaled,
    stage,
    part,
    part_in,
    sq,
    sq_in,
    bias_rows,
    fresh,
    att,
    att_in,
    update,
    fin,
    fsq_in,
    red,
    red_in,
    wq_sem,
    w_sem,
    part_s,
    part_r,
    sq_s,
    sq_r,
    att_s,
    att_r,
    hop_s,
    hop_r,
    fin_s,
    fin_r,
    sib_s,
    sib_r,
    fsq_s,
    fsq_r,
    fp_s,
    fp_r,
    red_s,
    red_r,
):
    sec = lax.axis_index("pipe")
    me = lax.axis_index("mp")
    total = sections * n
    rows, width = hidden.shape
    lc = kv.shape[0]
    heads_all = HEADS + 2 * KV_HEADS
    group = HEADS // KV_HEADS
    phases = heads_all // group
    span = lc * group
    last = sections - 1
    scale = HEAD_DIM ** (-0.5)
    cw = group * HEAD_DIM
    half = rows // 2
    core = lax.rem(sec, 2)
    sibling = sec + 1 - 2 * core

    def wq_copy(c):
        cols = pl.ds(pl.multiple_of(c * cw, cw), cw)
        return pltpu.make_async_copy(qkv_weight.at[0, :, cols], wq.at[:, cols], wq_sem.at[c])

    def phase_of(k):
        return lax.rem(k + phases - 1, phases)

    for k in range(phases):
        wq_copy((k + phases - 1) % phases).start()
    kv_copy = pltpu.make_async_copy(cache.at[0], kv, w_sem.at[0])
    wo_copy = pltpu.make_async_copy(out_weight.at[0], wo, w_sem.at[1])
    hw_copy = pltpu.make_async_copy(head_weight, hw, w_sem.at[2])

    @pl.when(sec > 0)
    def _():
        kv_copy.start()
        wo_copy.start()
        hw_copy.start()

    barrier = pltpu.get_barrier_semaphore()
    mine = sec * n + me

    def greet(k, carry):
        other = lax.rem(mine + k, total)
        pl.semaphore_signal(
            barrier, inc=1, device_id=(other // n, lax.rem(other, n)), device_id_type=MESH
        )
        return carry

    lax.fori_loop(1, total, greet, 0)

    for i in range(heads_all):
        bias_rows[i : i + 1, :] = bias[:, i * HEAD_DIM : (i + 1) * HEAD_DIM].astype(F32)
    eye = lax.broadcasted_iota(jnp.int32, (rows, 128), 0) == lax.broadcasted_iota(
        jnp.int32, (rows, 128), 1
    )

    def to_row(col):
        return jnp.sum(jnp.where(eye, col, 0.0), axis=0, keepdims=True)

    def to_col(row):
        return jnp.sum(jnp.where(eye, row, 0.0), axis=1, keepdims=True)

    small_eye = lax.broadcasted_iota(jnp.int32, (rows, rows), 0) == lax.broadcasted_iota(
        jnp.int32, (rows, rows), 1
    )
    assign_col = jnp.sum(
        jnp.where(small_eye, assign[...].astype(F32), 0.0), axis=1, keepdims=True
    )
    order = assign_col == lax.broadcasted_iota(jnp.int32, (rows, rows), 1).astype(F32)
    target = jnp.sum(
        jnp.where(order, token_ids[...].astype(F32), 0.0), axis=1, keepdims=True
    )
    lane = lax.broadcasted_iota(jnp.int32, (1, HEAD_DIM), 1)
    lane_rows = lax.broadcasted_iota(jnp.int32, (1, rows), 1)
    own_len = [
        jnp.sum(
            jnp.where(lane_rows == me * lc + i, lengths[...].astype(F32), 0.0),
            axis=1,
            keepdims=True,
        )
        for i in range(lc)
    ]
    angles = jnp.concatenate([length * freq[...] for length in own_len], axis=0)
    cosine = jnp.cos(angles)
    sine = jnp.sin(angles) * jnp.where(lane < HEAD_DIM // 2, -1.0, 1.0)

    pl.semaphore_wait(barrier, total - 1)

    @pl.when(sec == 0)
    def _():
        x[...] = hidden[...]

    @pl.when(sec > 0)
    def _():
        remote(xo, x, hop_s, hop_r, (sec - 1, me)).wait_recv()

    current = x[...].astype(F32)
    sq[...] = jnp.broadcast_to(
        to_row(jnp.sum(current * current, axis=1, keepdims=True)), sq.shape
    )
    scaled[...] = (current * gain[...].astype(F32)).astype(BF16)

    def sq_copy(peer, slot):
        return remote(sq, sq_in.at[slot], sq_s.at[peer], sq_r.at[slot], (sec, peer))

    def to_peer(k):
        return lax.rem(me + k, n)

    for k in range(1, n):
        sq_copy(to_peer(k), me).start()
    sq_in[me] = sq[...]

    def part_copy(phase, peer, slot):
        return remote(
            part.at[phase, peer],
            part_in.at[phase, slot],
            part_s.at[phase, peer],
            part_r.at[phase, slot],
            (sec, peer),
        )

    def project(k, carry):
        phase = phase_of(k)

        @pl.when((sec == 0) & (k == 2))
        def _():
            kv_copy.start()

        wq_copy(phase).wait()
        base = pl.multiple_of(phase * cw, cw)
        piece = jnp.dot(scaled[...], wq[:, pl.ds(base, cw)], preferred_element_type=F32)
        for j in range(group):
            stage[pl.ds(j, rows, stride=group), :] = piece[
                :, j * HEAD_DIM : (j + 1) * HEAD_DIM
            ]
        for p in range(n):
            part[phase, p] = stage[p * span : (p + 1) * span, :].astype(BF16)
        for k in range(1, n):
            part_copy(phase, to_peer(k), me).start()
        part_in[phase, me] = part[phase, me]
        return carry

    lax.fori_loop(0, phases, project, 0)

    @pl.when(sec == 0)
    def _():
        wo_copy.start()
        hw_copy.start()

    def from_peer(k):
        return lax.rem(me + n - k, n)

    def summed(phase):
        for k in range(1, n):
            peer = from_peer(k)
            part_copy(phase, peer, peer).wait_recv()
        result = part_in[phase, 0].astype(F32)
        for p in range(1, n):
            result = result + part_in[phase, p].astype(F32)
        return result

    for k in range(1, n):
        peer = from_peer(k)
        sq_copy(peer, peer).wait_recv()
    squares = sq_in[0]
    for p in range(1, n):
        squares = squares + sq_in[p]
    factor = [
        lax.rsqrt(
            jnp.sum(
                jnp.where(lane == me * lc + i, squares[0:1, :], 0.0), axis=1, keepdims=True
            )
            / (n * width)
            + EPS
        )
        for i in range(lc)
    ]

    def turn(block, i):
        return (
            block * cosine[i : i + 1]
            + pltpu.roll(block, HEAD_DIM // 2, 1) * sine[i : i + 1]
        )

    is_key = lax.broadcasted_iota(jnp.int32, (2 * KV_HEADS, HEAD_DIM), 0) < KV_HEADS
    block_sum = summed(phases - 1)
    for i in range(lc):
        block = block_sum[i * group : (i + 1) * group] * factor[i] + bias_rows[HEADS:, :]
        fresh[i] = jnp.where(is_key, turn(block, i), block).astype(BF16).astype(F32)
    kv_copy.wait()
    pos = lax.broadcasted_iota(jnp.int32, (1, kv.shape[3]), 1).astype(F32)

    def att_copy(h, peer, slot):
        return remote(
            att.at[h], att_in.at[h, slot], att_s.at[h, peer], att_r.at[h, slot], (sec, peer)
        )

    together = 2

    def attend(step, carry):
        sums = [summed(step * together + u) for u in range(together)]
        for u in range(together):
            h = step * together + u
            bias_h = bias_rows[pl.ds(pl.multiple_of(h * group, group), group), :]
            done = []
            for i in range(lc):
                block = sums[u][i * group : (i + 1) * group] * factor[i] + bias_h
                query = turn(block, i).astype(BF16)
                key_new = fresh[i, pl.ds(h, 1), :]
                value_new = fresh[i, pl.ds(KV_HEADS + h, 1), :]
                visible = pos < own_len[i]
                scores = (
                    lax.dot_general(
                        query,
                        kv[i, 0, h],
                        (((1,), (1,)), ((), ())),
                        preferred_element_type=F32,
                    )
                    * scale
                )
                self_score = (
                    jnp.sum(query.astype(F32) * key_new, axis=1, keepdims=True) * scale
                )
                top = jnp.maximum(
                    jnp.max(jnp.where(visible, scores, -1e30), axis=1, keepdims=True),
                    self_score,
                )
                weights = jnp.where(visible, jnp.exp(scores - top), 0.0)
                self_weight = jnp.exp(self_score - top)
                denominator = jnp.sum(weights, axis=1, keepdims=True) + self_weight
                mixed = jnp.dot(
                    weights.astype(BF16), kv[i, 1, h], preferred_element_type=F32
                )
                mixed = mixed + self_weight.astype(BF16).astype(F32) * value_new
                done.append(mixed / denominator)
            att[h] = jnp.concatenate(done, axis=0).astype(BF16)
            att_in[h, me] = att[h]
        for u in range(together):
            h = step * together + u
            for k in range(1, n):
                att_copy(h, to_peer(k), me).start()
        return carry

    lax.fori_loop(0, KV_HEADS // together, attend, 0)
    wo_copy.wait()
    update[...] = x[...].astype(F32)

    def project_out(h, carry):
        for k in range(1, n):
            peer = from_peer(k)
            att_copy(h, peer, peer).wait_recv()
        for p in range(n):
            stage[p * span : (p + 1) * span, :] = att_in[h, p].astype(F32)
        mat = jnp.concatenate(
            [stage[pl.ds(j, rows, stride=group), :].astype(BF16) for j in range(group)],
            axis=1,
        )
        depth = pl.ds(pl.multiple_of(h * cw, cw), cw)
        update[...] += jnp.dot(mat, wo[depth, :], preferred_element_type=F32)
        return carry

    lax.fori_loop(0, KV_HEADS, project_out, 0)
    xo[...] = update[...].astype(BF16)

    @pl.when(sec < last)
    def _():
        hop = remote(xo, x, hop_s, hop_r, (sec + 1, me))
        hop.start()
        hop.wait_send()

    def fin_pipe(k):
        to = lax.rem(sec + k, sections)
        piece = lax.rem(to, 2)
        return (
            remote(fin.at[piece, me], fin.at[piece, me], fp_s.at[2 * k], fp_r.at[0], (to, me)),
            remote(fsq_in.at[me], fsq_in.at[me], fp_s.at[2 * k + 1], fp_r.at[1], (to, me)),
        )

    @pl.when(sec == last)
    def _():
        final = jnp.dot(order.astype(BF16), xo[...], preferred_element_type=F32)
        both = (final * final_gain[...].astype(F32)[None, :]).astype(BF16)
        fin[0, me] = both[:half]
        fin[1, me] = both[half:]
        fsq_in[me] = jnp.broadcast_to(
            to_row(jnp.sum(final * final, axis=1, keepdims=True)), (8, 128)
        )
        for k in range(1, sections):
            for copy in fin_pipe(k):
                copy.start()

    @pl.when(sec < last)
    def _():
        arriving = remote(fin.at[core, me], fin.at[core, me], fp_s.at[0], fp_r.at[0], (last, me))
        arriving.wait_recv()
        arriving = remote(fsq_in.at[me], fsq_in.at[me], fp_s.at[1], fp_r.at[1], (last, me))
        arriving.wait_recv()

    def fin_copy(peer, slot):
        return remote(
            fin.at[core, slot], fin.at[core, slot], fin_s.at[peer], fin_r.at[slot], (sec, peer)
        )

    def sib_copy(piece, slot):
        return remote(
            fin.at[piece, slot], fin.at[piece, slot], sib_s.at[slot], sib_r.at[slot], (sibling, me)
        )

    def fsq_copy(peer, slot):
        return remote(
            fsq_in.at[slot], fsq_in.at[slot], fsq_s.at[peer], fsq_r.at[slot], (sec, peer)
        )

    for k in range(1, n):
        fin_copy(to_peer(k), me).start()
    for k in range(1, n):
        fsq_copy(to_peer(k), me).start()

    @pl.when(sec < last - 1)
    def _():
        sib_copy(core, me).start()

    @pl.when(sec == last - 1)
    def _():
        mate = remote(fin.at[1 - core, me], fin.at[1 - core, me], fp_s.at[0], fp_r.at[2], (last, me))
        mate.wait_recv()

    @pl.when(sec == last)
    def _():
        mate = remote(
            fin.at[core, me], fin.at[core, me], sib_s.at[me], fp_r.at[2], (sibling, me)
        )
        mate.start()

    for k in range(1, n):
        peer = from_peer(k)
        fin_copy(peer, peer).wait_recv()
        sib_copy(core, peer).start()

    @pl.when(sec < last - 1)
    def _():
        sib_copy(1 - core, me).wait_recv()

    hw_copy.wait()

    def head(k, logits):
        peer = from_peer(k)

        @pl.when(k > 0)
        def _():
            sib_copy(1 - core, peer).wait_recv()

        rows_at = pl.ds(pl.multiple_of(peer * width, width), width)
        both = jnp.concatenate([fin[0, peer], fin[1, peer]], axis=0)
        return logits + jnp.dot(both, hw[rows_at, :], preferred_element_type=F32)

    logits = lax.fori_loop(0, n, head, jnp.zeros(out.shape, F32))
    for k in range(1, n):
        peer = from_peer(k)
        fsq_copy(peer, peer).wait_recv()
    squares = fsq_in[0]
    for p in range(1, n):
        squares = squares + fsq_in[p]
    logits = logits * lax.rsqrt(to_col(squares[0:1, :]) / (n * width) + EPS)
    vocab = out.shape[1]
    ids = (mine * vocab + lax.broadcasted_iota(jnp.int32, (1, vocab), 1)).astype(F32)
    picked = jnp.sum(jnp.where(ids == target, logits, 0.0), axis=1, keepdims=True)
    top = jnp.max(logits, axis=1, keepdims=True)
    amount = jnp.sum(jnp.exp(logits - top), axis=1, keepdims=True)
    red[...] = jnp.concatenate(
        [to_row(top), to_row(amount), to_row(picked), jnp.zeros((5, 128), F32)], axis=0
    )

    def red_copy(other, slot):
        return remote(
            red,
            red_in.at[slot],
            red_s.at[other],
            red_r.at[slot],
            (other // n, lax.rem(other, n)),
        )

    def red_start(k, carry):
        red_copy(lax.rem(mine + k, total), mine).start()
        return carry

    lax.fori_loop(1, total, red_start, 0)
    red_in[mine] = red[...]

    def red_wait(k, carry):
        other = lax.rem(mine + total - k, total)
        red_copy(other, other).wait_recv()
        return carry

    lax.fori_loop(1, total, red_wait, 0)
    tops = red_in[:, 0, :]
    row_top = jnp.max(tops, axis=0, keepdims=True)
    row_total = jnp.sum(red_in[:, 1, :] * jnp.exp(tops - row_top), axis=0, keepdims=True)
    log_total = row_top + jnp.log(row_total)
    chosen[...] = jnp.sum(red_in[:, 2, :], axis=0, keepdims=True) - log_total
    out[...] = logits - to_col(log_total)

    def peer_done(k, carry):
        peer = to_peer(k)
        sq_copy(peer, me).wait_send()
        for phase in range(phases):
            part_copy(phase, peer, me).wait_send()
        for h in range(KV_HEADS):
            att_copy(h, peer, me).wait_send()
        fin_copy(peer, me).wait_send()
        fsq_copy(peer, me).wait_send()
        sib_copy(core, peer).wait_send()
        return carry

    lax.fori_loop(1, n, peer_done, 0)

    @pl.when(sec != last - 1)
    def _():
        sib_copy(core, me).wait_send()

    @pl.when(sec == last)
    def _():
        for k in range(1, sections):
            for copy in fin_pipe(k):
                copy.wait_send()

    def red_done(k, carry):
        red_copy(lax.rem(mine + k, total), mine).wait_send()
        return carry

    lax.fori_loop(1, total, red_done, 0)


def local(
    hidden_in,
    lengths,
    assign,
    token_ids,
    attn_gain,
    qkv_weight,
    qkv_bias,
    out_weight,
    kv_cache,
    final_gain,
    head_weight,
):
    sections = lax.axis_size("pipe")
    n = lax.axis_size("mp")
    rows, width = hidden_in.shape
    lc = kv_cache.shape[1]
    qkv = qkv_weight.shape[2]
    inner = out_weight.shape[1]
    vocab = head_weight.shape[1]
    heads_all = HEADS + 2 * KV_HEADS
    half = HEAD_DIM // 2
    frequency = np.float32(THETA) ** (
        -np.arange(half).astype(np.float32) * np.float32(2.0) / np.float32(HEAD_DIM)
    )
    freq = jnp.asarray(np.concatenate([frequency, frequency])[None, :], F32)
    group = HEADS // KV_HEADS
    phases = heads_all // group
    span = lc * group
    dma = pltpu.SemaphoreType.DMA
    vm = pl.BlockSpec(memory_space=pltpu.VMEM)
    hbm = pl.BlockSpec(memory_space=pl.ANY)
    total = sections * n
    logprobs, chosen = pl.pallas_call(
        functools.partial(kernel, sections, n),
        out_shape=(
            jax.ShapeDtypeStruct((rows, vocab), F32),
            jax.ShapeDtypeStruct((1, 128), F32),
        ),
        in_specs=[vm, vm, vm, vm, vm, hbm, vm, hbm, hbm, vm, hbm, vm],
        out_specs=(vm, vm),
        scratch_shapes=[
            pltpu.VMEM((width, qkv), BF16),
            pltpu.VMEM((inner, width), BF16),
            pltpu.VMEM(kv_cache.shape[1:], BF16),
            pltpu.VMEM(head_weight.shape, BF16),
            pltpu.VMEM((rows, width), BF16),
            pltpu.VMEM((rows, width), BF16),
            pltpu.VMEM((rows, width), BF16),
            pltpu.VMEM((rows * group, HEAD_DIM), F32),
            pltpu.VMEM((phases, n, span, HEAD_DIM), BF16),
            pltpu.VMEM((phases, n, span, HEAD_DIM), BF16),
            pltpu.VMEM((8, 128), F32),
            pltpu.VMEM((n, 8, 128), F32),
            pltpu.VMEM((heads_all, HEAD_DIM), F32),
            pltpu.VMEM((lc, 2 * KV_HEADS, HEAD_DIM), F32),
            pltpu.VMEM((KV_HEADS, span, HEAD_DIM), BF16),
            pltpu.VMEM((KV_HEADS, n, span, HEAD_DIM), BF16),
            pltpu.VMEM((rows, width), F32),
            pltpu.VMEM((2, n, rows // 2, width), BF16),
            pltpu.VMEM((n, 8, 128), F32),
            pltpu.VMEM((8, 128), F32),
            pltpu.VMEM((total, 8, 128), F32),
            dma((phases,)),
            dma((3,)),
            dma((phases, n)),
            dma((phases, n)),
            dma((n,)),
            dma((n,)),
            dma((KV_HEADS, n)),
            dma((KV_HEADS, n)),
            dma,
            dma,
            dma((n,)),
            dma((n,)),
            dma((n,)),
            dma((n,)),
            dma((n,)),
            dma((n,)),
            dma((2 * sections,)),
            dma((3,)),
            dma((total,)),
            dma((total,)),
        ],
        compiler_params=pltpu.CompilerParams(
            collective_id=0, has_side_effects=True, vmem_limit_bytes=60 * 1024 * 1024
        ),
    )(
        hidden_in,
        lengths.reshape(1, rows),
        assign.reshape(1, rows),
        token_ids.reshape(1, rows),
        attn_gain,
        qkv_weight,
        qkv_bias,
        out_weight,
        kv_cache,
        final_gain,
        head_weight,
        freq,
    )
    return logprobs, chosen[0, :rows]


def solution(mesh):
    return jax.shard_map(
        local,
        mesh=mesh,
        in_specs=(
            P(None, "mp"),
            P(),
            P(),
            P(),
            P("pipe", "mp"),
            P("pipe", "mp", None),
            P("pipe", None),
            P("pipe", None, "mp"),
            P("pipe", "mp", None, None, None, None),
            P("mp"),
            P(None, ("pipe", "mp")),
        ),
        out_specs=(P(None, ("pipe", "mp")), P()),
        check_vma=False,
    )
```
